8 devices in a mesh: pod: 1 (over z), data: 2 (over y), expert: 4 (over x, core).
Axes of the slice: x: 2, y: 2, z: 1, core: 2. Of those that a mesh axis runs over, the one named last changes fastest.
Arguments:
- tokens: bfloat16 [16384, 1024], P(('pod', 'data', 'expert'))
- routes: int32 [16384, 8], P(('pod', 'data', 'expert'))
- gates: float32 [16384, 8], P(('pod', 'data', 'expert'))
- grad_y: bfloat16 [16384, 1024], P(('pod', 'data', 'expert'))
- w_in1: bfloat16 [32, 1024, 512], P('expert')
- w_in3: bfloat16 [32, 1024, 512], P('expert')
- w_out: bfloat16 [32, 512, 1024], P('expert')
Outputs:
- output 1: bfloat16 [16384, 1024], P(('pod', 'data', 'expert'))
- output 2: bfloat16 [16384, 1024], P(('pod', 'data', 'expert'))
- output 3: float32 [32, 1024, 512], P(('pod', 'expert'))
- output 4: float32 [32, 1024, 512], P(('pod', 'expert'))
- output 5: float32 [32, 512, 1024], P(('pod', 'expert'))
All inputs are finite; a program needn't handle non-finite values.
Results may differ from the reference program's by a relative error of at most 0.0102961.
Values are sent between devices in bfloat16 or wider.
A program may use at most 1 GiB of HBM per device.

```python
import functools
import jax
import jax.numpy as jnp
from jax import lax

D_MODEL = 1024
D_FF = 512
N_EXPERTS = 32
TOP_K = 8
TOK_DEV = 2048
N_DATA = 2
N_EXPERT_DEV = 4
CAP_COLD = 496
CAP_HOT = 768
N_HOT = 2

GROUPS = N_DATA * N_EXPERT_DEV
TOK_PART = GROUPS * TOK_DEV


def hot_index_table(expert_ids):
    return jnp.where(expert_ids == 0, 0, jnp.where(expert_ids == N_EXPERTS // 2, 1, -1))


def draw_routes(key):
    key_hot, key_pos, key_base_a, key_base_b, key_step = jax.random.split(key, 5)
    n_cold = N_EXPERTS - N_HOT
    pattern = jnp.concatenate([
        jnp.zeros((CAP_HOT,), jnp.int32),
        jnp.ones((CAP_HOT,), jnp.int32),
        jnp.full((TOK_DEV - N_HOT * CAP_HOT,), -1, jnp.int32)])
    hot_of_tok = jax.random.permutation(key_hot, pattern)
    hot_slot = jax.random.randint(key_pos, (TOK_DEV, 1), 0, TOP_K)
    base_rank = jnp.minimum(jax.random.randint(key_base_a, (TOK_DEV, 1), 0, n_cold),
                            jax.random.randint(key_base_b, (TOK_DEV, 1), 0, n_cold))
    step_max = max(1, (n_cold - 1) // max(TOP_K - 1, 1))
    step_size = jax.random.randint(key_step, (TOK_DEV, 1), 1, step_max + 1)
    slot_ids = jnp.arange(TOP_K)[None, :]
    cold_rank = (base_rank + slot_ids * step_size) % n_cold
    cold_expert = cold_rank + 1 + (cold_rank + 1 >= N_EXPERTS // 2).astype(jnp.int32)
    use_hot = (hot_of_tok[:, None] >= 0) & (slot_ids == hot_slot)
    return jnp.where(use_hot, hot_of_tok[:, None] * (N_EXPERTS // 2), cold_expert).astype(jnp.int32)


def setup_inputs(seed: int = 0, part: int = 0) -> dict:
    key = jax.random.key(seed)
    key_part = jax.random.fold_in(key, part)
    key_tok, key_route, key_gate, key_grad = jax.random.split(key_part, 4)
    key_one, key_three, key_two = jax.random.split(jax.random.fold_in(key, 99991), 3)
    routes = jax.vmap(draw_routes)(jax.random.split(key_route, GROUPS)).reshape(TOK_PART, TOP_K)
    tokens = jax.random.normal(key_tok, (TOK_PART, D_MODEL), jnp.float32).astype(jnp.bfloat16)
    gates = jax.random.uniform(key_gate, (TOK_PART, TOP_K), jnp.float32, 0.5, 1.5)
    grad_y = jax.random.normal(key_grad, (TOK_PART, D_MODEL), jnp.float32).astype(jnp.bfloat16)
    w_in1 = (jax.random.normal(key_one, (N_EXPERTS, D_MODEL, D_FF), jnp.float32) * D_MODEL ** -0.5).astype(jnp.bfloat16)
    w_in3 = (jax.random.normal(key_three, (N_EXPERTS, D_MODEL, D_FF), jnp.float32) * D_MODEL ** -0.5).astype(jnp.bfloat16)
    w_out = (jax.random.normal(key_two, (N_EXPERTS, D_FF, D_MODEL), jnp.float32) * D_FF ** -0.5).astype(jnp.bfloat16)
    return dict(tokens=tokens, routes=routes, gates=gates, grad_y=grad_y, w_in1=w_in1, w_in3=w_in3, w_out=w_out)


def route_rows(routes_dev):
    flat_exp = routes_dev.reshape(-1)
    n_slots = flat_exp.shape[0]
    order = jnp.argsort(flat_exp, stable=True)
    counts = jax.ops.segment_sum(jnp.ones((n_slots,), jnp.int32), flat_exp, num_segments=N_EXPERTS)
    starts = jnp.cumsum(counts) - counts
    rank_sorted = jnp.arange(n_slots, dtype=jnp.int32) - starts[flat_exp[order]]
    slot_rank = jnp.zeros((n_slots,), jnp.int32).at[order].set(rank_sorted)
    hot_index = hot_index_table(flat_exp)
    cold_row = jnp.where((hot_index < 0) & (slot_rank < CAP_COLD), flat_exp * CAP_COLD + slot_rank, N_EXPERTS * CAP_COLD)
    hot_row = jnp.where(hot_index >= 0, hot_index * CAP_HOT + slot_rank, N_HOT * CAP_HOT)
    return cold_row, hot_row


def gather_rows(slot_rows, x_local, dy_local, gate_flat, n_rows):
    n_slots = slot_rows.shape[0]
    tok_n = x_local.shape[0]
    top_k = n_slots // tok_n
    src_tok = jnp.full((n_rows,), tok_n, jnp.int32).at[slot_rows].set(
        jnp.arange(n_slots, dtype=jnp.int32) // top_k, mode='drop')
    src_gate = jnp.zeros((n_rows,), jnp.float32).at[slot_rows].set(gate_flat, mode='drop')
    x_rows = jnp.take(x_local, src_tok, axis=0, mode='fill', fill_value=0)
    dy_rows = jnp.take(dy_local, src_tok, axis=0, mode='fill', fill_value=0)
    do_rows = (dy_rows.astype(jnp.float32) * src_gate[:, None]).astype(jnp.bfloat16)
    return x_rows, do_rows


def expert_pass(x_rows, do_rows, w_a, w_b, w_c):
    pre_a = jnp.dot(x_rows, w_a, preferred_element_type=jnp.float32).astype(jnp.bfloat16)
    pre_b = jnp.dot(x_rows, w_b, preferred_element_type=jnp.float32).astype(jnp.bfloat16)
    act_a = pre_a.astype(jnp.float32)
    act_b = pre_b.astype(jnp.float32)
    sigma_a = jax.nn.sigmoid(act_a)
    hidden = (act_a * sigma_a * act_b).astype(jnp.bfloat16)
    outs = jnp.dot(hidden, w_c, preferred_element_type=jnp.float32).astype(jnp.bfloat16)
    d_hidden = jnp.dot(do_rows, w_c.T, preferred_element_type=jnp.float32)
    d_pre_b = (d_hidden * act_a * sigma_a).astype(jnp.bfloat16)
    d_pre_a = (d_hidden * act_b * sigma_a * (1.0 + act_a * (1.0 - sigma_a))).astype(jnp.bfloat16)
    d_rows = (jnp.dot(d_pre_a, w_a.T, preferred_element_type=jnp.float32)
              + jnp.dot(d_pre_b, w_b.T, preferred_element_type=jnp.float32)).astype(jnp.bfloat16)
    grad_a = jnp.dot(x_rows.T, d_pre_a, preferred_element_type=jnp.float32)
    grad_b = jnp.dot(x_rows.T, d_pre_b, preferred_element_type=jnp.float32)
    grad_c = jnp.dot(hidden.T, do_rows, preferred_element_type=jnp.float32)
    return outs, d_rows, grad_a, grad_b, grad_c


def run_expert(operands):
    return expert_pass(*operands)


def combine(cold_rows, hot_rows, cold_vals, hot_vals, weights):
    slot_vals = (jnp.take(cold_vals, cold_rows, axis=0, mode='fill', fill_value=0)
                 + jnp.take(hot_vals, hot_rows, axis=0, mode='fill', fill_value=0))
    weighted = weights.reshape(TOK_DEV, TOP_K, 1) * slot_vals.reshape(TOK_DEV, TOP_K, D_MODEL).astype(jnp.float32)
    return jnp.sum(weighted, axis=1).astype(jnp.bfloat16)


def by_expert(buffers, n_buf, cap):
    return buffers.reshape(GROUPS, n_buf, cap, D_MODEL).transpose(1, 0, 2, 3).reshape(n_buf, GROUPS * cap, D_MODEL)


def by_device(buffers, n_buf, cap):
    return buffers.reshape(n_buf, GROUPS, cap, D_MODEL).transpose(1, 0, 2, 3).reshape(GROUPS, n_buf * cap, D_MODEL)


def reference(tokens, routes, gates, grad_y, w_in1, w_in3, w_out):
    x_dev = tokens.reshape(GROUPS, TOK_DEV, D_MODEL)
    dy_dev = grad_y.reshape(GROUPS, TOK_DEV, D_MODEL)
    gate_dev = gates.reshape(GROUPS, TOK_DEV * TOP_K)
    cold_row, hot_row = jax.vmap(route_rows)(routes.reshape(GROUPS, TOK_DEV, TOP_K))
    cold_x, cold_do = jax.vmap(functools.partial(gather_rows, n_rows=N_EXPERTS * CAP_COLD))(cold_row, x_dev, dy_dev, gate_dev)
    hot_x, hot_do = jax.vmap(functools.partial(gather_rows, n_rows=N_HOT * CAP_HOT))(hot_row, x_dev, dy_dev, gate_dev)
    hot_ids = jnp.array([0, N_EXPERTS // 2])
    cold_out, cold_dx, grad_one, grad_three, grad_two = lax.map(run_expert, (
        by_expert(cold_x, N_EXPERTS, CAP_COLD), by_expert(cold_do, N_EXPERTS, CAP_COLD), w_in1, w_in3, w_out))
    hot_out, hot_dx, hot_one, hot_three, hot_two = lax.map(run_expert, (
        by_expert(hot_x, N_HOT, CAP_HOT), by_expert(hot_do, N_HOT, CAP_HOT),
        w_in1[hot_ids], w_in3[hot_ids], w_out[hot_ids]))
    y_out = jax.vmap(combine)(cold_row, hot_row, by_device(cold_out, N_EXPERTS, CAP_COLD),
                              by_device(hot_out, N_HOT, CAP_HOT), gate_dev)
    grad_x = jax.vmap(combine)(cold_row, hot_row, by_device(cold_dx, N_EXPERTS, CAP_COLD),
                               by_device(hot_dx, N_HOT, CAP_HOT), jnp.ones_like(gate_dev))
    return (y_out.reshape(TOK_PART, D_MODEL), grad_x.reshape(TOK_PART, D_MODEL),
            grad_one.at[hot_ids].add(hot_one), grad_three.at[hot_ids].add(hot_three),
            grad_two.at[hot_ids].add(hot_two))
```

```python
import functools

import jax
import jax.numpy as jnp
from jax import lax
from jax.experimental import pallas as pl
from jax.experimental.pallas import tpu as pltpu
from jax.sharding import PartitionSpec as P


N_EXP = 32
TOK = 2048
D = 1024
F = 512
LANES = 128
CH = D // LANES
TOP_K = 8
SLOTS = TOK * TOP_K
CAP_COLD = 496
CAP_HOT = 768
CAPS = (CAP_HOT, CAP_COLD, CAP_COLD, CAP_COLD)
LIST = SLOTS + 1024
UNROLL = 8
BF = jnp.bfloat16
F32 = jnp.float32


def gather_kernel(meta, idx, gate, x_ref, dy_ref, *rest):
    x0, x1, d0, d1, xs, ds = rest[-6:]
    g = pl.program_id(0)
    for pos, rows in enumerate(CAPS):
        start = meta[g * 4 + pos]
        cnt = meta[8 + g * 4 + pos]

        def group(i0, carry):
            for u in range(UNROLL):
                i = i0 * UNROLL + u
                t = idx[start + i]
                gt = gate[start + i]
                at = pl.ds(pl.multiple_of(i * CH, CH), CH)
                xs[at, :] = x_ref[t].astype(F32)
                ds[at, :] = dy_ref[t].astype(F32) * gt
            return carry

        lax.fori_loop(0, rows // UNROLL, group, 0)
        live = lax.broadcasted_iota(jnp.int32, (rows, LANES), 0) < cnt
        for k in range(CH):
            xk = xs[pl.ds(k, rows, stride=CH), :].astype(BF)
            dk = jnp.where(live, ds[pl.ds(k, rows, stride=CH), :], 0.0).astype(BF)
            lanes = slice(k * LANES, (k + 1) * LANES)
            if pos == 0:
                x0[0, 0, :, lanes] = xk
                d0[0, 0, :, lanes] = dk
            else:
                x1[0, 0, pos - 1, :, lanes] = xk
                d1[0, 0, pos - 1, :, lanes] = dk


def gather_rows(s, n_src, n_grp, table, x3, dy3, prev):
    meta, idx, gate = table
    smem = pl.BlockSpec(memory_space=pltpu.SMEM)
    whole = pl.BlockSpec((TOK, CH, LANES), lambda g: (0, 0, 0))
    shapes = [jax.ShapeDtypeStruct((n_src, n_grp, CAP_HOT, D), BF),
              jax.ShapeDtypeStruct((n_src, n_grp, 3, CAP_COLD, D), BF)] * 2
    specs = [pl.BlockSpec((1, 1, CAP_HOT, D), lambda g: (s, g, 0, 0)),
             pl.BlockSpec((1, 1, 3, CAP_COLD, D), lambda g: (s, g, 0, 0, 0))] * 2
    args = [meta, idx, gate, x3, dy3]
    in_specs = [smem, smem, smem, whole, whole]
    alias = {}
    if prev is not None:
        alias = {5 + i: i for i in range(4)}
        args += list(prev)
        in_specs += [pl.BlockSpec(memory_space=pl.ANY)] * 4
    return pl.pallas_call(
        gather_kernel, grid=(n_grp,), out_shape=shapes, in_specs=in_specs, out_specs=specs,
        input_output_aliases=alias,
        scratch_shapes=[pltpu.VMEM((CAP_HOT * CH, LANES), F32)] * 2,
        cost_estimate=pl.CostEstimate(flops=n_grp * 10 ** 10, bytes_accessed=n_grp * 10 ** 7, transcendentals=0),
        name="gather_rows",
    )(*args)


def dot(a, b, dims):
    return lax.dot_general(a, b, (dims, ((), ())), preferred_element_type=F32)


NN = ((1,), (0,))
NT = ((1,), (1,))
TN = ((0,), (0,))


def expert_rows(x, do, w1, w3, w2, o, dx, g13, g2):
    pre_a = dot(x, w1, NN).astype(BF)
    pre_b = dot(x, w3, NN).astype(BF)
    dh = dot(do, w2, NT)
    a = pre_a.astype(F32)
    b = pre_b.astype(F32)
    sig = jax.nn.sigmoid(a)
    hid = (a * sig * b).astype(BF)
    db = (dh * a * sig).astype(BF)
    da = (dh * b * sig * (1.0 + a * (1.0 - sig))).astype(BF)
    if o is not None:
        o[...] = dot(hid, w2, NN).astype(BF).reshape(o.shape)
        dx[...] = (dot(da, w1, NT) + dot(db, w3, NT)).astype(BF).reshape(dx.shape)
    if g13 is not None:
        g13[0] += dot(x, da, TN)
        g13[1] += dot(x, db, TN)
        g2[...] += dot(hid, do, TN)


def mine_kernel(first, n_out, q_ref, x, d, fx, fd, w1, w3, w2, *rest):
    outs, g13, g2 = rest[-2 - n_out:-2], rest[-2], rest[-1]
    s = pl.program_id(0)

    @pl.when(s == 0)
    def _():
        g13[...] = jnp.zeros_like(g13)
        g2[...] = jnp.zeros_like(g2)

    rows = x.shape[-2]
    weights = (w1.at[0], w3.at[0], w2.at[0])

    def run(xr, dr, o, dx):
        expert_rows(xr[...].reshape(rows, D), dr[...].reshape(rows, D), *[w[...] for w in weights], o, dx, g13, g2)

    if first == 0:
        @pl.when(s < 2)
        def _():
            run(x, d, outs[0], outs[1])

        @pl.when((s >= 2) & (s < 4))
        def _():
            run(x, d, outs[2], outs[3])
    else:
        @pl.when(s < 2)
        def _():
            run(x, d, None, None)

        @pl.when((s >= 2) & (s < 4))
        def _():
            run(x, d, outs[0], outs[1])

    @pl.when(s >= 4)
    def _():
        run(fx, fd, None, None)


def other_kernel(q_ref, x, d, w1, w3, w2, *rest):
    o, dx = rest[-2:]
    rows = x.shape[-2]
    expert_rows(x[...].reshape(rows, D), d[...].reshape(rows, D), w1[0], w3[0], w2[0], o, dx, None, None)


def w_specs(expert_of):
    return [pl.BlockSpec((1, D, F), lambda *a: (expert_of(*a), 0, 0)),
            pl.BlockSpec((1, D, F), lambda *a: (expert_of(*a), 0, 0)),
            pl.BlockSpec((1, F, D), lambda *a: (expert_of(*a), 0, 0))]


def row_spec(pos, grp, src_of):
    if pos == 0:
        return pl.BlockSpec((1, 1, CAP_HOT, D), lambda *a: (src_of(*a), grp, 0, 0))
    return pl.BlockSpec((1, 1, 1, CAP_COLD, D), lambda *a: (src_of(*a), grp, pos - 1, 0, 0))


def row_shape(pos):
    if pos == 0:
        return jax.ShapeDtypeStruct((2, 2, CAP_HOT, D), BF)
    return jax.ShapeDtypeStruct((2, 2, 3, CAP_COLD, D), BF)


VMEM_LIMIT = 63 * 1024 * 1024


def run_mine(pos, first, q1, x, d, fx, fd, weights, prev):
    own = lambda s, q: jnp.minimum(s, 3)
    far = lambda s, q: jnp.maximum(s - 4, 0)
    near = lambda s, q: jnp.clip(s - 2, 0, 1)
    exp = lambda s, q: q[0] * 4 + pos
    in_specs = [row_spec(pos, 0, own)] * 2 + [row_spec(pos, 0, far)] * 2 + w_specs(exp)
    args = [x, d, fx, fd, *weights]
    out_specs = [row_spec(pos, 0, near)] * 2
    if first == 0:
        out_specs = [row_spec(pos, 0, lambda s, q: jnp.minimum(s, 1))] * 2 + out_specs
    n_out = len(out_specs)
    alias = {}
    if prev is not None:
        alias = {8 + i: i for i in range(n_out)}
        args += list(prev)
        in_specs += [pl.BlockSpec(memory_space=pl.ANY)] * n_out
    rows = CAPS[pos]
    return pl.pallas_call(
        functools.partial(mine_kernel, first, n_out),
        grid_spec=pltpu.PrefetchScalarGridSpec(
            num_scalar_prefetch=1, grid=(8,), in_specs=in_specs,
            out_specs=out_specs + [
                pl.BlockSpec((2, D, F), lambda s, q: (0, 0, 0)),
                pl.BlockSpec((F, D), lambda s, q: (0, 0))]),
        out_shape=[row_shape(pos)] * n_out + [jax.ShapeDtypeStruct((2, D, F), F32),
                                              jax.ShapeDtypeStruct((F, D), F32)],
        input_output_aliases=alias,
        compiler_params=pltpu.CompilerParams(vmem_limit_bytes=VMEM_LIMIT),
        cost_estimate=pl.CostEstimate(flops=2 * rows * 4 * 15 * D * F, bytes_accessed=rows * 50000, transcendentals=0),
        name="mine",
    )(q1, *args)


def run_other(pos0, n_pos, grp, first, q1, x, d, weights, prev):
    exp = lambda p, s, q: (q[0] if grp == 0 else 1 - q[0]) * 4 + pos0 + p

    def spec(s0):
        if pos0 == 0:
            return pl.BlockSpec((1, 1, CAP_HOT, D), lambda p, s, q: (s0 + s, grp, 0, 0))
        return pl.BlockSpec((1, 1, 1, CAP_COLD, D), lambda p, s, q: (s0 + s, grp, pos0 - 1 + p, 0, 0))

    in_specs = [spec(first)] * 2 + w_specs(exp)
    args = [x, d, *weights]
    alias = {}
    if prev is not None:
        alias = {6: 0, 7: 1}
        args += list(prev)
        in_specs += [pl.BlockSpec(memory_space=pl.ANY)] * 2
    rows = CAPS[pos0] * n_pos
    return pl.pallas_call(
        other_kernel,
        grid_spec=pltpu.PrefetchScalarGridSpec(
            num_scalar_prefetch=1, grid=(n_pos, 2), in_specs=in_specs, out_specs=[spec(0)] * 2),
        out_shape=[row_shape(pos0)] * 2,
        input_output_aliases=alias,
        compiler_params=pltpu.CompilerParams(vmem_limit_bytes=VMEM_LIMIT),
        cost_estimate=pl.CostEstimate(flops=2 * rows * 2 * 6 * D * F, bytes_accessed=rows * 25000, transcendentals=0),
        name="other",
    )(q1, *args)


def combine_kernel(gated, has_init, meta, idx, gate, *rest):
    if has_init:
        init, rest = rest[0], rest[1:]
    o0, o1, out, acc, rows_f, sem = rest
    g = pl.program_id(0)
    main = acc.at[pl.ds(0, TOK)]

    @pl.when(g == 0)
    def _():
        if has_init:
            copy = pltpu.make_async_copy(init, main, sem.at[0])
            copy.start()
            copy.wait()
            acc[pl.ds(TOK, UNROLL)] = jnp.zeros((UNROLL, CH, LANES), F32)
        else:
            acc[...] = jnp.zeros_like(acc)

    for pos, rows in enumerate(CAPS):
        start = meta[g * 4 + pos]
        cnt = meta[8 + g * 4 + pos]
        for k in range(CH):
            lanes = slice(k * LANES, (k + 1) * LANES)
            ok = o0[0, 0, :, lanes] if pos == 0 else o1[0, 0, pos - 1, :, lanes]
            rows_f[pl.ds(k, rows, stride=CH), :] = ok.astype(F32)

        def group(i0, carry):
            base = i0 * UNROLL
            toks = [jnp.where(base + u < cnt, idx[start + base + u], TOK + u) for u in range(UNROLL)]
            vals = [rows_f[pl.ds(pl.multiple_of((base + u) * CH, CH), CH), :] for u in range(UNROLL)]
            if gated:
                vals = [v * gate[start + base + u] for u, v in enumerate(vals)]
            sums = [acc[t] + v for t, v in zip(toks, vals)]
            for t, v in zip(toks, sums):
                acc[t] = v
            return carry

        lax.fori_loop(0, (cnt + UNROLL - 1) // UNROLL, group, 0)

    @pl.when(g == 1)
    def _():
        copy = pltpu.make_async_copy(main, out, sem.at[0])
        copy.start()
        copy.wait()


def combine(s, table, rows, gated, init):
    meta, idx, gate = table
    smem = pl.BlockSpec(memory_space=pltpu.SMEM)
    anym = pl.BlockSpec(memory_space=pl.ANY)
    r0 = pl.BlockSpec((1, 1, CAP_HOT, D), lambda g: (s, g, 0, 0))
    r1 = pl.BlockSpec((1, 1, 3, CAP_COLD, D), lambda g: (s, g, 0, 0, 0))
    args = [meta, idx, gate] + ([init] if init is not None else []) + list(rows)
    in_specs = [smem] * 3 + ([anym] if init is not None else []) + [r0, r1]
    return pl.pallas_call(
        functools.partial(combine_kernel, gated, init is not None), grid=(2,),
        out_shape=jax.ShapeDtypeStruct((TOK, CH, LANES), F32),
        in_specs=in_specs, out_specs=anym,
        scratch_shapes=[pltpu.VMEM((TOK + UNROLL, CH, LANES), F32), pltpu.VMEM((CAP_HOT * CH, LANES), F32),
                        pltpu.SemaphoreType.DMA((1,))],
        compiler_params=pltpu.CompilerParams(vmem_limit_bytes=VMEM_LIMIT),
        cost_estimate=pl.CostEstimate(flops=2 * 10 ** 10, bytes_accessed=2 * 10 ** 7, transcendentals=0),
        name="combine",
    )(*args)


def slot_lists(routes, gates):
    flat = routes.reshape(-1)
    key = flat * SLOTS + jnp.arange(SLOTS, dtype=jnp.int32)
    key, gate = lax.sort((key, gates.reshape(-1)), num_keys=1, is_stable=False)
    tok = (key % SLOTS) // TOP_K
    exps = jnp.arange(N_EXP, dtype=jnp.int32)
    counts = jnp.sum((routes[:, :, None] == exps).astype(jnp.int32), axis=(0, 1))
    starts = jnp.sum(jnp.where(exps[None, :] < exps[:, None], counts[None, :], 0), axis=1)
    hot = (exps == 0) | (exps == N_EXP // 2)
    kept = jnp.minimum(counts, jnp.where(hot, CAP_HOT, CAP_COLD))
    pad = jnp.zeros((LIST - SLOTS,), F32)
    return jnp.concatenate([tok.astype(F32), pad, gate, pad, starts.astype(F32), kept.astype(F32)])


def solution(mesh):
    row_spec_p = P(('pod', 'data', 'expert'), None)
    w_spec = P('expert', None, None)
    grad_spec = P(('pod', 'expert'), None, None)

    def core(v):
        return lax.ppermute(v, 'expert', [(i, i ^ 1) for i in range(4)])

    def xhop(v):
        return lax.ppermute(v, 'expert', [(i, i ^ 2) for i in range(4)])

    def yhop(v):
        return lax.ppermute(v, 'data', [(0, 1), (1, 0)])

    def body(tokens, routes, gates, grad_y, w_in1, w_in3, w_out):
        q = lax.axis_index('data')
        r = lax.axis_index('expert')
        q1 = q.reshape(1).astype(jnp.int32)

        x = [tokens.reshape(TOK, CH, LANES)] + [None] * 7
        dy = [grad_y.reshape(TOK, CH, LANES)] + [None] * 7
        x[0], dy[0], routes, gates = lax.optimization_barrier((x[0], dy[0], routes, gates))
        for v in (x, dy):
            v[2] = xhop(v[0])
            v[4] = yhop(v[0])
            v[1] = core(v[0])
        x[6] = xhop(x[4])
        dy[6] = yhop(dy[2])
        for v in (x, dy):
            v[3] = core(v[2])
            v[5] = core(v[4])
            v[7] = core(v[6])

        lists = lax.all_gather(slot_lists(routes, gates), ('data', 'expert'))

        def table(s):
            src = (q ^ (s // 4)) * 4 + (r ^ (s % 4))
            row = lax.dynamic_index_in_dim(lists, src, 0, keepdims=False)
            idx = row[:LIST].astype(jnp.int32)
            bounds = row[2 * LIST:].reshape(2, 4, 2, 4)
            bounds = lax.dynamic_index_in_dim(bounds, r, 1, keepdims=False)
            bounds = jnp.where(q == 0, bounds, bounds[:, ::-1])
            return bounds.reshape(-1).astype(jnp.int32), idx, row[LIST:2 * LIST]

        tables = [table(s) for s in range(8)]

        own = far = None
        for place, src in ((2, 0), (3, 1), (0, 2), (1, 3)):
            own = gather_rows(place, 4, 2, tables[src], x[src], dy[src], own)
        for s in range(4):
            far = gather_rows(s, 4, 1, tables[4 + s], x[4 + s], dy[4 + s], far)
        weights = (w_in1, w_in3, w_out)
        own0, own1 = (own[0], own[2]), (own[1], own[3])
        far0, far1 = (far[0], far[2]), (far[1], far[3])

        *out1, a13, a2 = run_mine(1, 0, q1, *own1, *far1, weights, None)
        *out1, b13, b2 = run_mine(2, 0, q1, *own1, *far1, weights, out1)
        out_a1, out_b1 = out1[:2], out1[2:]
        out_a1 = run_other(3, 1, 0, 0, q1, *own1, weights, out_a1)
        out_a0 = run_other(0, 1, 0, 0, q1, *own0, weights, None)
        out_a0 = run_other(0, 1, 1, 0, q1, *own0, weights, out_a0)
        out_a1 = run_other(1, 3, 1, 0, q1, *own1, weights, out_a1)

        rows_y, rows_d = (out_a0[0], out_a1[0]), (out_a0[1], out_a1[1])
        far_y = core(combine(1, tables[3], rows_y, True, None))
        far_d = core(combine(1, tables[3], rows_d, False, None))
        far_y = xhop(combine(0, tables[2], rows_y, True, far_y))
        far_d = xhop(combine(0, tables[2], rows_d, False, far_d))

        *out_b1, c13, c2 = run_mine(3, 2, q1, *own1, *far1, weights, out_b1)
        *out_b0, d13, d2 = run_mine(0, 2, q1, *own0, *far0, weights, None)
        out_b0 = run_other(0, 1, 1, 2, q1, *own0, weights, out_b0)
        out_b1 = run_other(1, 3, 1, 2, q1, *own1, weights, out_b1)
        rows_y, rows_d = (out_b0[0], out_b1[0]), (out_b0[1], out_b1[1])
        home_y = core(combine(1, tables[1], rows_y, True, None))
        home_d = core(combine(1, tables[1], rows_d, False, None))
        home_y = combine(0, tables[0], rows_y, True, home_y)
        home_d = combine(0, tables[0], rows_d, False, home_d)
        y_out = (home_y + far_y).astype(BF).reshape(TOK, D)
        grad_x = (home_d + far_d).astype(BF).reshape(TOK, D)

        grads = [None] * 4
        for pos, g13, g2 in ((1, a13, a2), (2, b13, b2), (3, c13, c2), (0, d13, d2)):
            grads[pos] = (g13, g2, yhop(g13), yhop(g2))
        grad_1 = jnp.zeros((8, D, F), F32)
        grad_3 = jnp.zeros((8, D, F), F32)
        grad_2 = jnp.zeros((8, F, D), F32)
        for pos in (1, 2, 3, 0):
            g13, g2, h13, h2 = grads[pos]
            for base, v13, v2 in ((q * 4, g13, g2), ((1 - q) * 4, h13, h2)):
                at = (base + pos, 0, 0)
                grad_1 = lax.dynamic_update_slice(grad_1, v13[:1], at)
                grad_3 = lax.dynamic_update_slice(grad_3, v13[1:], at)
                grad_2 = lax.dynamic_update_slice(grad_2, v2[None], at)
        return y_out, grad_x, grad_1, grad_3, grad_2

    return jax.shard_map(body, mesh=mesh,
                         in_specs=(row_spec_p, row_spec_p, row_spec_p, row_spec_p, w_spec, w_spec, w_spec),
                         out_specs=(row_spec_p, row_spec_p, grad_spec, grad_spec, grad_spec),
                         check_vma=False)
```
